32 devices in a mesh: grp: 4 (over y, x), mem: 8 (over z, core).
Axes of the slice: x: 2, y: 2, z: 4, core: 2. Of those that a mesh axis runs over, the one named last changes fastest.
Arguments:
- weight: bfloat16 [2, 16384, 16384], P(None, None, ('grp', 'mem')), may hold values from -0.046875 to 0.046875
- activation: bfloat16 [2, 16384, 512], P(None, ('grp', 'mem')), may hold values from -6 to 6
- points: int32 [4], replicated, may hold values from 0 to 3, each once
Outputs:
- share: float32 [4, 16384, 512], P('grp', 'mem')
The draws below stay inside these ranges and needn't reach their ends.
Inputs may be any that keep to these rules, and one draw needn't show every extreme that they name: A permutation of 0 to 3; group g evaluates at points[g] + 1.
All inputs are finite; a program needn't handle non-finite values.
Results may differ from the reference program's by a relative error of at most 0.0042.
Values may be sent and summed in bfloat16 or wider, within the bound.
A program may use at most 320 MiB of HBM per device.

```python
import jax
import jax.numpy as jnp

D = 16384
C = 512
SPLITS = 2
BLOCKS = 2
FB = 16384
N_GRP = 4


def steps_of(own_key, extent, cuts, low, high):
    level = 1.0
    for dim, blocks in cuts:
        steps = jax.random.uniform(jax.random.fold_in(jax.random.fold_in(own_key, 6), dim), (blocks,), jnp.float32, low / len(cuts), high / len(cuts))
        level = level * jnp.repeat(jnp.exp(steps), extent[dim] // blocks).reshape((-1,) + (1,) * (len(extent) - 1 - dim))
    return level


def scatter_about(stream_key, dims, width, bound, cuts=(), held_as=jnp.bfloat16):
    entries = width * jax.random.normal(stream_key, dims, jnp.float32)
    if cuts:
        entries = entries * steps_of(stream_key, dims, cuts, -0.22, 0.18)
    return jnp.clip(entries, -bound, bound).astype(held_as)


def setup_inputs(seed: int = 0) -> dict:
    keys = jax.random.split(jax.random.key(seed), 4)
    weight = scatter_about(keys[0], (BLOCKS, FB, D), D ** -0.5, 0.046875, ((2, 32),))
    activation = scatter_about(keys[1], (SPLITS, D, C), 1.0, 6.0, ((1, 32),))
    points = jax.random.permutation(keys[2], N_GRP).astype(jnp.int32)
    return {"weight": weight, "activation": activation, "points": points}


def reference(weight, activation, points):
    anchors = (points + 1).astype(jnp.float32) / N_GRP
    weight_powers = jnp.arange(BLOCKS, dtype=jnp.float32)
    input_powers = jnp.arange(SPLITS, dtype=jnp.float32) * BLOCKS
    shares = []
    for group in range(N_GRP):
        factors = anchors[group] ** weight_powers
        total = factors[0] * weight[0].astype(jnp.float32)
        for block in range(1, BLOCKS):
            total = total + factors[block] * weight[block].astype(jnp.float32)
        coded_weight = total.astype(jnp.bfloat16)
        lifts = anchors[group] ** input_powers
        mixed = lifts[0] * activation[0].astype(jnp.float32)
        for split in range(1, SPLITS):
            mixed = mixed + lifts[split] * activation[split].astype(jnp.float32)
        coded_input = mixed.astype(jnp.bfloat16)
        shares.append(jnp.dot(coded_weight, coded_input, preferred_element_type=jnp.float32))
    return jnp.stack(shares)
```

```python
import jax
import jax.numpy as jnp
from jax import lax
from jax.experimental import pallas as pl
from jax.experimental.pallas import tpu as pltpu
from jax.sharding import PartitionSpec as P

SHARE_A = 14
SHARES_B = (15, 15, 13, 7)
LIMIT = 58 * 1024 * 1024
UNITS_A = ((4, 2), (3, 2), (3, 3), (0, 0))
F32, BF16 = jnp.float32, jnp.bfloat16
MESH = pl.DeviceIdType.MESH


def loop(n, body):
    def step(i, carry):
        body(i)
        return carry

    lax.fori_loop(0, n, step, 0)


def blend(o, v0, v1):
    return v0 + o * (v1 - v0)


def choose(values, index):
    width = len(values)
    while width > 1:
        bit = index % 2
        values = [blend(bit, values[2 * i], values[2 * i + 1]) for i in range(width // 2)]
        index, width = index // 2, width // 2
    return values[0]


def line_order(n):
    table = []
    for z in range(n):
        def key(d):
            up = d > z
            slot = (n - 1 - d) + z if up else d + (n - 1 - z)
            return slot, up == (z < n // 2)
        table.append(sorted([d for d in range(n) if d != z], key=key) + [z])
    return table


def make_kernel(groups, members, blocks, splits, rows, depth, cols, ra, rbs):
    bits = groups.bit_length() - 1
    ring = members // 2
    half = groups // 2
    pairs = len(rbs)
    top = max([ra] + rbs)
    leads = [2 * ra + 2 * sum(rbs[:p]) for p in range(pairs)]
    off = [groups - (groups >> s) for s in range(bits + 1)]
    order_of = line_order(ring)
    n_units = 4 * ring

    def kernel(*refs):
        points, weight, act, out, wxa = refs[:5]
        wxb = refs[5:5 + pairs]
        refs = refs[5 + pairs:]
        (xo, xp, xs, wt, cw, accs, az, ag, bsend, x_s, x_r, x_o, w_s, wa_r, ld, send, b_s, az_r, ag_s, ag_r) = refs[:20]
        refs = refs[20:]
        bg, bz = refs[:pairs], refs[pairs:2 * pairs]
        wb_r, bg_r, bz_r = (refs[(2 + k) * pairs:(3 + k) * pairs] for k in range(3))

        me_g = lax.axis_index("grp")
        me_m = lax.axis_index("mem")
        z, core = me_m // 2, me_m % 2
        twin = (me_g, z * 2 + 1 - core)

        def bit_of(w):
            return (me_g // w) % 2

        def across(o, s):
            w0, w1 = 1 << (bits - 1 - s), 1 << s
            p0 = me_g + w0 - 2 * w0 * bit_of(w0)
            p1 = me_g + w1 - 2 * w1 * bit_of(w1)
            return (blend(o, p0, p1), me_m)

        def group_at(o, s, h, j):
            w0, w1 = 1 << (bits - 1 - s), 1 << s
            b0, b1 = bit_of(w0), bit_of(w1)
            b0, b1 = b0 + h - 2 * b0 * h, b1 + h - 2 * b1 * h
            g0 = (me_g // (2 * w0)) * (2 * w0) + b0 * w0 + j
            g1 = me_g % w1 + b1 * w1 + j * (2 * w1)
            return blend(o, g0, g1)

        def slot_at(o, s, h, j):
            w0, w1 = 1 << (bits - 1 - s), 1 << s
            b0, b1 = bit_of(w0), bit_of(w1)
            b0, b1 = b0 + h - 2 * b0 * h, b1 + h - 2 * b1 * h
            return blend(o, b0 * w0 + j, b1 + 2 * j)

        def remote(src, dst, ssem, rsem, dev):
            return pltpu.make_async_remote_copy(
                src_ref=src, dst_ref=dst, send_sem=ssem, recv_sem=rsem, device_id=dev, device_id_type=MESH)

        def arrived(ref, sem):
            pltpu.make_async_copy(ref, ref, sem).wait()

        def anchor(g):
            return (points[g] + 1).astype(F32) / groups

        def power(a, n):
            r = a
            for _ in range(n - 1):
                r = r * a
            return r

        def per_place(fn):
            return [choose([fn(q, order_of[q][t]) for q in range(ring)], z) for t in range(ring)]

        def landing(q, d):
            if d == q:
                return d
            return ring if d == q - 1 else d

        dests = per_place(lambda q, d: d)
        signs = per_place(lambda q, d: 1 if d > q else -1)
        feeds = per_place(lambda q, d: int(d != q and 0 <= q - (1 if d > q else -1) < ring))
        lands = per_place(landing)
        left, right = z > 0, z < ring - 1
        ends = choose([int(q in (0, ring - 1)) for q in range(ring)], z)

        def dest(t):
            return dests[t] if isinstance(t, int) else choose(dests, t)

        def toward(t):
            return (me_g, (z + choose(signs, t)) * 2 + core)

        barrier = pltpu.get_barrier_semaphore()
        peers = [twin] + [across(0, s) for s in range(bits)]
        for dev in peers:
            pl.semaphore_signal(barrier, inc=1, device_id=dev, device_id_type=MESH)
        for there, sgn in ((left, -1), (right, 1)):
            @pl.when(there)
            def _(sgn=sgn):
                pl.semaphore_signal(barrier, inc=1, device_id=(me_g, (z + sgn) * 2 + core), device_id_type=MESH)

        def meet():
            beside = choose([int(q > 0) + int(q < ring - 1) for q in range(ring)], z)
            pl.semaphore_wait(barrier, len(peers) + beside)

        x_own = pltpu.make_async_copy(act, xo, x_o)
        x_own.start()

        def base(lead, d, core_):
            return pl.multiple_of((d * 2 + core_) * rows + lead, 16)

        x_copy = remote(act, xp, x_s, x_r, twin)

        def push_a(c, t):
            remote(weight.at[:, pl.ds(base(c * ra, dest(t), 1 - core), ra), :], wxa.at[c, t],
                   w_s.at[pairs], wa_r.at[c, t], twin).start()

        def push_b(p, c, t):
            rb = rbs[p]
            remote(weight.at[:, pl.ds(base(leads[p] + c * rb, dest(t), 1 - core), rb), :], wxb[p].at[c, t],
                   w_s.at[p], wb_r[p].at[c, t], twin).start()

        def push_both(p):
            def body(i):
                push_b(p, i % 2, i // 2)
            loop(2 * ring, body)

        def push_first(t):
            push_a(0, t)
            push_b(0, 0, t)
            push_b(0, 1, t)

        step = min(16, depth)
        lifts = [power(anchor(g), blocks) for g in range(groups)]

        def code_input(h, src):
            def body(r):
                at = pl.ds(pl.multiple_of(r * step, step), step)
                to = pl.ds(pl.multiple_of(h * depth + r * step, step), step)
                parts = [src[k, at, :].astype(F32) for k in range(splits)]
                for g in range(groups):
                    total = parts[0]
                    for k in range(1, splits):
                        total = total + power(lifts[g], k) * parts[k]
                    xs[g, to, :] = total.astype(BF16)
            loop(depth // step, body)

        meet()
        x_copy.start()
        loop(ring, push_first)
        x_own.wait()
        code_input(0, xo)

        def tile_copies(lead, d, n, there, slot):
            own = pltpu.make_async_copy(
                weight.at[:, pl.ds(base(lead, d, core), n), :], wt.at[slot, 0, :, pl.ds(0, n), :], ld.at[slot, 0])
            other = pltpu.make_async_copy(there, wt.at[slot, 1, :, pl.ds(0, n), :], ld.at[slot, 1])
            return own, other

        def product(slot, n, g):
            a = anchor(g)
            factors = [power(a, j) for j in range(1, blocks)]

            def body(r):
                at = pl.ds(r * 16, 16)
                for h in range(2):
                    total = wt[slot, h, 0, at, :].astype(F32)
                    for j in range(1, blocks):
                        total = total + factors[j - 1] * wt[slot, h, j, at, :].astype(F32)
                    cw[at, h * depth:(h + 1) * depth] = total.astype(BF16)
            for r in range(n // 16):
                body(r)
            return jnp.dot(cw[0:n, :], xs[g], preferred_element_type=F32)

        def a_unit(u):
            return u // (2 * ring), (u // 2) % ring, u % 2

        def a_body(u, slot):
            c, t, hh = a_unit(u)
            d, feed = dest(t), choose(feeds, t)
            last = t == ring - 1

            def per_group(j):
                g = group_at(c, 0, 1 - hh, j)
                accs[0:ra, :] = product(slot, ra, g)

                def take(there, at):
                    @pl.when(there)
                    def _():
                        arrived(az.at[c, at, g], az_r.at[c, at, g])
                        accs[0:ra, :] = accs[0:ra, :] + az[c, at, g].astype(F32)

                take(jnp.logical_or(feed == 1, jnp.logical_and(last, left)), d)
                take(jnp.logical_and(last, right), ring)
                az[c, d, g] = accs[0:ra, :].astype(BF16)

                @pl.when(t < ring - 1)
                def _():
                    land = choose(lands, t)
                    remote(az.at[c, d, g], az.at[c, land, g], send.at[0], az_r.at[c, land, g], toward(t)).start()
            loop(half, per_group)

        def a_spread(c):
            n = half // 2

            def per_slot(i):
                j = slot_at(c, 1, 1 - i // n, i % n)
                g = group_at(c, 0, 1, j)
                remote(az.at[c, z, g], ag.at[c, j], send.at[1], ag_s.at[c, j], across(c, 0)).start()
            loop(half, per_slot)

        def a_held(s, c, j):
            if s == 1:
                return az[c, z, group_at(c, 0, 0, j)]
            return ag[c, off[s - 2] + slot_at(c, s - 1, 0, j)]

        def a_sum(s, c, j):
            return ag[c, off[s - 1] + j].astype(F32) + a_held(s, c, j).astype(F32)

        def a_part(s, c, h):
            n = half >> s

            def per_slot(jj):
                j = slot_at(c, s, h, jj)
                if s == 1:
                    arrived(ag.at[c, j], ag_s.at[c, j])
                ag[c, off[s - 1] + j] = a_sum(s, c, j).astype(BF16)
                if h == 1:
                    remote(ag.at[c, off[s - 1] + j], ag.at[c, off[s] + jj], send.at[2],
                           ag_r.at[c, s], across(c, s)).start()
            loop(n, per_slot)

        def a_send(s, c):
            if s > 1:
                arrived(ag.at[c, pl.ds(off[s - 1], half >> (s - 1))], ag_r.at[c, s - 1])
            a_part(s, c, 1)

        def a_keep(s, c):
            a_part(s, c, 0)

        def a_close(c):
            arrived(ag.at[c, pl.ds(off[bits - 1], 1)], ag_r.at[c, bits - 1])
            out[0, pl.ds(pl.multiple_of(c * ra, 16), ra), :] = a_sum(bits, c, 0)

        def b_first(p, c, t, slot):
            rb, q = rbs[p], p % 2

            def per_slot(j):
                acc = product(slot, rb, group_at(c, 0, 1, j))
                src = bsend.at[q, c, t, j, pl.ds(0, rb), :]
                src[...] = acc.astype(BF16)
                remote(src, bg[p].at[c, t, j], b_s.at[q], bg_r[p].at[c, t, 0], across(c, 0)).start()
            loop(half, per_slot)

        def b_sent(p):
            q = p % 2
            arrived(bsend.at[q, :, :, :, pl.ds(0, rbs[p]), :], b_s.at[q])

        def b_merge(p, c, t, s, add):
            n = half >> (s - 1)
            arrived(bg[p].at[c, t, pl.ds(off[s - 1], n)], bg_r[p].at[c, t, s - 1])

            def per_slot(i):
                h, jj = 1 - i // (n // 2), i % (n // 2)
                j = slot_at(c, s, h, jj)
                bg[p][c, t, off[s - 1] + j] = (add(j) + bg[p][c, t, off[s - 1] + j].astype(F32)).astype(BF16)

                @pl.when(i < n // 2)
                def _():
                    remote(bg[p].at[c, t, off[s - 1] + j], bg[p].at[c, t, off[s] + jj], send.at[3],
                           bg_r[p].at[c, t, s], across(c, s)).start()
            loop(n, per_slot)

        def b_second(p, c, t, slot):
            b_merge(p, c, t, 1, lambda j: product(slot, rbs[p], group_at(c, 0, 0, j)))

        def b_middle(p, t):
            for s in range(2, bits):
                loop(2, lambda c: b_merge(
                    p, c, t, s, lambda j: bg[p][c, t, off[s - 2] + slot_at(c, s - 1, 0, j)].astype(F32)))

        def b_line(p, t):
            rb = rbs[p]
            d = dest(t)

            def body(c):
                tail = off[bits - 1]
                arrived(bg[p].at[c, t, pl.ds(tail, 1)], bg_r[p].at[c, t, bits - 1])
                kept = off[bits - 2] + slot_at(c, bits - 1, 0, 0)

                def val():
                    return bg[p][c, t, tail].astype(F32) + bg[p][c, t, kept].astype(F32)

                feed = choose(feeds, t)
                mid = t < ring - 1

                @pl.when(jnp.logical_and(mid, feed == 0))
                def _():
                    bz[p][c, d] = val().astype(BF16)

                @pl.when(jnp.logical_and(mid, feed == 1))
                def _():
                    arrived(bz[p].at[c, d], bz_r[p].at[c, d])
                    bz[p][c, d] = (val() + bz[p][c, d].astype(F32)).astype(BF16)

                @pl.when(mid)
                def _():
                    land = choose(lands, t)
                    remote(bz[p].at[c, d], bz[p].at[c, land], send.at[4], bz_r[p].at[c, land], toward(t)).start()

                @pl.when(t == ring - 1)
                def _():
                    at = pl.ds(pl.multiple_of(leads[p] + c * rb, 16), rb)
                    out[0, at, :] = val()
                    for there, slot in ((left, z), (right, ring)):
                        @pl.when(there)
                        def _():
                            arrived(bz[p].at[c, slot], bz_r[p].at[c, slot])
                            out[0, at, :] = out[0, at, :] + bz[p][c, slot].astype(F32)
            loop(2, body)

        class Tiles:
            def __init__(self, count, spot, body, first=None, valid=None):
                self.count, self.spot, self.body, self.first = count, spot, body, first
                self.valid = valid or (lambda i: None)

            def guard(self, i, fn):
                ok = self.valid(i)
                if ok is None:
                    fn()
                else:
                    pl.when(ok)(fn)

            def begin(self, i, j, slot):
                def go():
                    own, other = tile_copies(*self.spot(i, j), slot)
                    own.start()
                    if self.first is not None:
                        self.first(i, j)
                    other.start()
                self.guard(i, go)

            def run(self, i, j, slot):
                def go():
                    for cp in tile_copies(*self.spot(i, j), slot):
                        cp.wait()
                    self.body(i, j, slot)
                self.guard(i, go)

        def b_tiles(p, first):
            rb = rbs[p]

            def spot(i, j):
                return leads[p] + j * rb, dest(i), rb, wxb[p].at[j, i]

            def await_rows(i, j):
                arrived(wxb[p].at[j, i], wb_r[p].at[j, i])

            fn = b_first if first else b_second
            return Tiles(2, spot, lambda i, j, slot: fn(p, j, i, slot), await_rows if first else None)

        def a_tiles(k0, amount, count):
            def unit(i):
                return k0 + (i * amount) // count - 1 + 2 * ends

            def spot(i, j):
                c, t, _ = a_unit(unit(i))
                return c * ra, dest(t), ra, wxa.at[c, t]

            def await_rows(i, j):
                c, t, hh = a_unit(unit(i))

                @pl.when(hh == 0)
                def _():
                    arrived(wxa.at[c, t], wa_r.at[c, t])

            def valid(i):
                u = unit(i)
                ok = jnp.logical_and(u >= 0, u < n_units)
                return jnp.logical_and(ok, ((i + 1) * amount) // count > (i * amount) // count)

            return Tiles(1, spot, lambda i, j, slot: a_body(unit(i), slot), await_rows, valid)

        def z_step(p, t):
            b_middle(p, t)
            b_line(p, t)

        early = a_tiles(-1, 1, 1)
        early.begin(0, 0, 0)
        b_tiles(0, True).begin(0, 0, 1)
        x_copy.wait_recv()
        code_input(1, xp)
        early.run(0, 0, 0)
        push_both(1)
        loop(ring, lambda t: push_a(1, t))
        for p in range(2, pairs):
            push_both(p)

        sites = []
        k0 = 0
        for p in range(pairs):
            final = p == pairs - 1
            for first in (True, False):
                amount = UNITS_A[p][0 if first else 1] * ring // 4
                parts = [b_tiles(p, first)]
                if amount:
                    parts.append(a_tiles(k0, amount, ring))
                    k0 += amount
                post = None
                if first and p >= 2:
                    sites.append(lambda p=p: b_sent(p - 2))
                if not first and p >= 1:
                    def post(i, p=p, final=final):
                        t = blend(ends, i - 1, i + 1)
                        ok = jnp.logical_and(t >= 0, t < ring - 1)

                        @pl.when(jnp.logical_and(ok, ends == 0) if final else ok)
                        def _():
                            z_step(p - 1, t)
                sites.append((ring, parts, post))
                if first and p >= 2:
                    sites.append(lambda p=p: z_step(p - 2, ring - 1))
                if first and p >= 1:
                    def lead_on(p=p, final=final):
                        @pl.when(ends == 1)
                        def _():
                            loop(ring - 1 if final else 1, lambda t: z_step(p - 1, t))
                    sites.append(lead_on)

        def tail():
            last = pairs - 1
            a_spread(0)
            a_spread(1)
            loop(ring - 2, lambda t: z_step(last, t))
            for c in range(2):
                a_send(1, c)
            z_step(last, ring - 2)
            for c in range(2):
                a_keep(1, c)
            z_step(last - 1, ring - 1)
            for s in range(2, bits):
                for c in range(2):
                    a_send(s, c)
                    a_keep(s, c)
            z_step(last, ring - 1)
            for c in range(2):
                a_close(c)

        sites.append(tail)

        tiled = [site for site in sites if isinstance(site, tuple)]
        seen, parity = 0, 1
        for site in sites:
            if not isinstance(site, tuple):
                site()
                continue
            seen += 1
            follow = tiled[seen][1][0] if seen < len(tiled) else None
            count, parts, post = site
            per = sum(part.count for part in parts)

            def run(i, count=count, parts=parts, post=post, per=per, follow=follow, parity=parity):
                lead = 0
                for q, part in enumerate(parts):
                    def visit(j, q=q, part=part, lead=lead):
                        slot = (parity + i * per + lead + j) % 2

                        @pl.when(j + 1 < part.count)
                        def _():
                            part.begin(i, j + 1, 1 - slot)

                        @pl.when(j + 1 == part.count)
                        def _():
                            if q + 1 < len(parts):
                                parts[q + 1].begin(i, 0, 1 - slot)
                                return

                            @pl.when(i + 1 < count)
                            def _():
                                parts[0].begin(i + 1, 0, 1 - slot)
                            if follow is not None:
                                @pl.when(i + 1 == count)
                                def _():
                                    follow.begin(0, 0, 1 - slot)
                        part.run(i, j, slot)
                    loop(part.count, visit)
                    lead += part.count
                if post is not None:
                    post(i)
            loop(count, run)
            parity = (parity + count * per) % 2

        x_copy.wait_send()
        for p in range(pairs):
            arrived(wxb[p], w_s.at[p])
        arrived(wxa, w_s.at[pairs])
        arrived(az.at[:, pl.ds(0, ring - 1)], send.at[0])
        arrived(ag.at[:, pl.ds(0, half)], send.at[1])
        arrived(ag.at[:, pl.ds(0, half - 1)], send.at[2])
        for p in range(max(0, pairs - 2), pairs):
            b_sent(p)
        for p in range(pairs):
            arrived(bg[p].at[:, :, pl.ds(0, half - 1)], send.at[3])
            arrived(bz[p].at[:, pl.ds(0, ring - 1)], send.at[4])

    dma = pltpu.SemaphoreType.DMA
    shapes = [
        pltpu.VMEM((splits, depth, cols), BF16),
        pltpu.VMEM((splits, depth, cols), BF16),
        pltpu.VMEM((groups, 2 * depth, cols), BF16),
        pltpu.VMEM((2, 2, blocks, top, depth), BF16),
        pltpu.VMEM((top, 2 * depth), BF16),
        pltpu.VMEM((top, cols), F32),
        pltpu.VMEM((2, ring + 1, groups, ra, cols), BF16),
        pltpu.VMEM((2, groups - 1, ra, cols), BF16),
        pltpu.VMEM((2, 2, ring, half, max(rbs), cols), BF16),
        dma, dma, dma, dma((pairs + 1,)), dma((2, ring)), dma((2, 2)), dma((5,)), dma((2,)),
        dma((2, ring + 1, groups)), dma((2, half)), dma((2, bits)),
    ]
    shapes += [pltpu.VMEM((2, ring, groups - 1, rb, cols), BF16) for rb in rbs]
    shapes += [pltpu.VMEM((2, ring + 1, rb, cols), BF16) for rb in rbs]
    shapes += [dma((2, ring)) for _ in rbs]
    shapes += [dma((2, ring, bits)) for _ in rbs]
    shapes += [dma((2, ring + 1)) for _ in rbs]
    held = [jax.ShapeDtypeStruct((2, ring, blocks, ra, depth), BF16)]
    held += [jax.ShapeDtypeStruct((2, ring, blocks, rb, depth), BF16) for rb in rbs]
    return pl.pallas_call(
        kernel,
        name="coded_share",
        out_shape=(pltpu.VMEM((1, rows, cols), F32), *held),
        in_specs=[
            pl.BlockSpec(memory_space=pltpu.SMEM),
            pl.BlockSpec(memory_space=pl.ANY),
            pl.BlockSpec(memory_space=pl.ANY),
        ],
        out_specs=tuple(pl.BlockSpec(memory_space=m) for m in [pltpu.VMEM] + [pl.ANY] * len(held)),
        scratch_shapes=shapes,
        compiler_params=pltpu.CompilerParams(
            collective_id=0, has_side_effects=True, vmem_limit_bytes=LIMIT),
    )


def split_rows(rows):
    units = rows // 16
    ua = max(1, units * SHARE_A // 128)
    ub = (units - 2 * ua) // 2
    whole = sum(SHARES_B)
    cut = [max(1, ub * share // whole) for share in SHARES_B]
    for i in range(ub - sum(cut)):
        cut[i % len(cut)] += 1
    return 16 * ua, [16 * n for n in cut]


def solution(mesh):
    groups, members = mesh.shape["grp"], mesh.shape["mem"]

    def per_device(weight, activation, points):
        blocks, height, depth = weight.shape
        splits, _, cols = activation.shape
        rows = height // members
        ra, rbs = split_rows(rows)
        call = make_kernel(groups, members, blocks, splits, rows, depth, cols, ra, rbs)
        return call(points, weight, activation)[0]

    placed = (P(None, None, ("grp", "mem")), P(None, ("grp", "mem"), None), P())
    return jax.shard_map(
        per_device, mesh=mesh, in_specs=placed, out_specs=P("grp", "mem", None), check_vma=False)
```

```python
import jax
import jax.numpy as jnp
from jax import lax
from jax.experimental import pallas as pl
from jax.experimental.pallas import tpu as pltpu
from jax.sharding import PartitionSpec as P

SHARE_A = 14
SHARES_B = (15, 15, 13, 7)
LIMIT = 58 * 1024 * 1024
UNITS_A = ((4, 3), (3, 2), (3, 3), (0, 0))
F32, BF16 = jnp.float32, jnp.bfloat16
MESH = pl.DeviceIdType.MESH


def loop(n, body):
    def step(i, carry):
        body(i)
        return carry

    lax.fori_loop(0, n, step, 0)


def blend(o, v0, v1):
    return v0 + o * (v1 - v0)


def choose(values, index):
    width = len(values)
    while width > 1:
        bit = index % 2
        values = [blend(bit, values[2 * i], values[2 * i + 1]) for i in range(width // 2)]
        index, width = index // 2, width // 2
    return values[0]


def line_order(n):
    table = []
    for z in range(n):
        def key(d):
            up = d > z
            slot = (n - 1 - d) + z if up else d + (n - 1 - z)
            return slot, up == (z < n // 2)
        table.append(sorted([d for d in range(n) if d != z], key=key) + [z])
    return table


def make_kernel(groups, members, blocks, splits, rows, depth, cols, ra, rbs):
    bits = groups.bit_length() - 1
    ring = members // 2
    half = groups // 2
    pairs = len(rbs)
    top = max([ra] + rbs)
    leads = [2 * ra + 2 * sum(rbs[:p]) for p in range(pairs)]
    off = [groups - (groups >> s) for s in range(bits + 1)]
    order_of = line_order(ring)
    n_units = 4 * ring

    def kernel(*refs):
        points, weight, act, out, wxa = refs[:5]
        wxb = refs[5:5 + pairs]
        refs = refs[5 + pairs:]
        (xo, xp, stage, xs, wt, cw, accs, az, ag, bsend, x_s, x_r, x_o, st_l, st_s, st_r, w_s, wa_r, ld, send, b_s, az_r, ag_s, ag_r) = refs[:24]
        refs = refs[24:]
        bg, bz = refs[:pairs], refs[pairs:2 * pairs]
        wb_r, bg_r, bz_r = (refs[(2 + k) * pairs:(3 + k) * pairs] for k in range(3))

        me_g = lax.axis_index("grp")
        me_m = lax.axis_index("mem")
        z, core = me_m // 2, me_m % 2
        twin = (me_g, z * 2 + 1 - core)

        def bit_of(w):
            return (me_g // w) % 2

        def across(o, s):
            w0, w1 = 1 << (bits - 1 - s), 1 << s
            p0 = me_g + w0 - 2 * w0 * bit_of(w0)
            p1 = me_g + w1 - 2 * w1 * bit_of(w1)
            return (blend(o, p0, p1), me_m)

        def group_at(o, s, h, j):
            w0, w1 = 1 << (bits - 1 - s), 1 << s
            b0, b1 = bit_of(w0), bit_of(w1)
            b0, b1 = b0 + h - 2 * b0 * h, b1 + h - 2 * b1 * h
            g0 = (me_g // (2 * w0)) * (2 * w0) + b0 * w0 + j
            g1 = me_g % w1 + b1 * w1 + j * (2 * w1)
            return blend(o, g0, g1)

        def slot_at(o, s, h, j):
            w0, w1 = 1 << (bits - 1 - s), 1 << s
            b0, b1 = bit_of(w0), bit_of(w1)
            b0, b1 = b0 + h - 2 * b0 * h, b1 + h - 2 * b1 * h
            return blend(o, b0 * w0 + j, b1 + 2 * j)

        def remote(src, dst, ssem, rsem, dev):
            return pltpu.make_async_remote_copy(
                src_ref=src, dst_ref=dst, send_sem=ssem, recv_sem=rsem, device_id=dev, device_id_type=MESH)

        def arrived(ref, sem):
            pltpu.make_async_copy(ref, ref, sem).wait()

        def anchor(g):
            return (points[g] + 1).astype(F32) / groups

        def power(a, n):
            r = a
            for _ in range(n - 1):
                r = r * a
            return r

        def per_place(fn):
            return [choose([fn(q, order_of[q][t]) for q in range(ring)], z) for t in range(ring)]

        def landing(q, d):
            if d == q:
                return d
            return ring if d == q - 1 else d

        dests = per_place(lambda q, d: d)
        signs = per_place(lambda q, d: 1 if d > q else -1)
        feeds = per_place(lambda q, d: int(d != q and 0 <= q - (1 if d > q else -1) < ring))
        lands = per_place(landing)
        left, right = z > 0, z < ring - 1
        ends = choose([int(q in (0, ring - 1)) for q in range(ring)], z)

        def dest(t):
            return dests[t] if isinstance(t, int) else choose(dests, t)

        def toward(t):
            return (me_g, (z + choose(signs, t)) * 2 + core)

        def base(lead, d, core_):
            return pl.multiple_of((d * 2 + core_) * rows + lead, 16)

        def tile_own(lead, d, n, there, slot):
            return pltpu.make_async_copy(
                weight.at[:, pl.ds(base(lead, d, core), n), :], wt.at[slot, 0, :, pl.ds(0, n), :], ld.at[slot, 0])

        def tile_other(lead, d, n, there, slot):
            return pltpu.make_async_copy(there, wt.at[slot, 1, :, pl.ds(0, n), :], ld.at[slot, 1])

        def stage_load(c):
            rb = rbs[0]
            return pltpu.make_async_copy(
                weight.at[:, pl.ds(base(leads[0] + c * rb, dest(0), 1 - core), rb), :], stage.at[c], st_l.at[c])

        def stage_give(c):
            return remote(stage.at[c], wt.at[c, 1, :, pl.ds(0, rbs[0]), :], st_s.at[c], st_r.at[c], twin)

        def begin_first():
            for c in range(2):
                stage_load(c).start()
                tile_own(leads[0] + c * rbs[0], dest(0), rbs[0], None, c).start()

        barrier = pltpu.get_barrier_semaphore()
        peers = [twin] + [across(0, s) for s in range(bits)]
        for dev in peers:
            pl.semaphore_signal(barrier, inc=1, device_id=dev, device_id_type=MESH)
        for there, sgn in ((left, -1), (right, 1)):
            @pl.when(there)
            def _(sgn=sgn):
                pl.semaphore_signal(barrier, inc=1, device_id=(me_g, (z + sgn) * 2 + core), device_id_type=MESH)

        def meet():
            beside = choose([int(q > 0) + int(q < ring - 1) for q in range(ring)], z)
            pl.semaphore_wait(barrier, len(peers) + beside)

        x_own = pltpu.make_async_copy(act, xo, x_o)
        x_own.start()
        begin_first()

        x_copy = remote(xo, xp, x_s, x_r, twin)

        def push_a(c, t):
            remote(weight.at[:, pl.ds(base(c * ra, dest(t), 1 - core), ra), :], wxa.at[c, t],
                   w_s.at[pairs], wa_r.at[c, t], twin).start()

        def push_b(p, c, t):
            rb = rbs[p]
            remote(weight.at[:, pl.ds(base(leads[p] + c * rb, dest(t), 1 - core), rb), :], wxb[p].at[c, t],
                   w_s.at[p], wb_r[p].at[c, t], twin).start()

        def push_both(p):
            def body(i):
                push_b(p, i % 2, i // 2)
            loop(2 * ring, body)

        def push_first(t):
            push_a(0, t)
            push_b(0, 0, (t + 1) % ring)
            push_b(0, 1, (t + 1) % ring)

        step = min(16, depth)
        lifts = [power(anchor(g), blocks) for g in range(groups)]

        def code_input(h, src):
            def body(r):
                at = pl.ds(pl.multiple_of(r * step, step), step)
                to = pl.ds(pl.multiple_of(h * depth + r * step, step), step)
                parts = [src[k, at, :].astype(F32) for k in range(splits)]
                for g in range(groups):
                    total = parts[0]
                    for k in range(1, splits):
                        total = total + power(lifts[g], k) * parts[k]
                    xs[g, to, :] = total.astype(BF16)
            loop(depth // step, body)

        x_own.wait()
        code_input(0, xo)
        for c in range(2):
            stage_load(c).wait()
        meet()
        x_copy.start()
        for c in range(2):
            stage_give(c).start()
        loop(ring, push_first)

        def product(slot, n, g):
            a = anchor(g)
            factors = [power(a, j) for j in range(1, blocks)]

            def body(r):
                at = pl.ds(r * 16, 16)
                for h in range(2):
                    total = wt[slot, h, 0, at, :].astype(F32)
                    for j in range(1, blocks):
                        total = total + factors[j - 1] * wt[slot, h, j, at, :].astype(F32)
                    cw[at, h * depth:(h + 1) * depth] = total.astype(BF16)
            for r in range(n // 16):
                body(r)
            return jnp.dot(cw[0:n, :], xs[g], preferred_element_type=F32)

        def a_unit(u):
            return u // (2 * ring), (u // 2) % ring, u % 2

        def a_body(u, slot):
            c, t, hh = a_unit(u)
            d, feed = dest(t), choose(feeds, t)
            last = t == ring - 1

            def per_group(j):
                g = group_at(c, 0, 1 - hh, j)
                accs[0:ra, :] = product(slot, ra, g)

                def take(there, at):
                    @pl.when(there)
                    def _():
                        arrived(az.at[c, at, g], az_r.at[c, at, g])
                        accs[0:ra, :] = accs[0:ra, :] + az[c, at, g].astype(F32)

                take(jnp.logical_or(feed == 1, jnp.logical_and(last, left)), d)
                take(jnp.logical_and(last, right), ring)
                az[c, d, g] = accs[0:ra, :].astype(BF16)

                @pl.when(t < ring - 1)
                def _():
                    land = choose(lands, t)
                    remote(az.at[c, d, g], az.at[c, land, g], send.at[0], az_r.at[c, land, g], toward(t)).start()
            loop(half, per_group)

        def a_spread(c):
            n = half // 2

            def per_slot(i):
                j = slot_at(c, 1, 1 - i // n, i % n)
                g = group_at(c, 0, 1, j)
                remote(az.at[c, z, g], ag.at[c, j], send.at[1], ag_s.at[c, j], across(c, 0)).start()
            loop(half, per_slot)

        def a_held(s, c, j):
            if s == 1:
                return az[c, z, group_at(c, 0, 0, j)]
            return ag[c, off[s - 2] + slot_at(c, s - 1, 0, j)]

        def a_sum(s, c, j):
            return ag[c, off[s - 1] + j].astype(F32) + a_held(s, c, j).astype(F32)

        def a_part(s, c, h):
            n = half >> s

            def per_slot(jj):
                j = slot_at(c, s, h, jj)
                if s == 1:
                    arrived(ag.at[c, j], ag_s.at[c, j])
                ag[c, off[s - 1] + j] = a_sum(s, c, j).astype(BF16)
                if h == 1:
                    remote(ag.at[c, off[s - 1] + j], ag.at[c, off[s] + jj], send.at[2],
                           ag_r.at[c, s], across(c, s)).start()
            loop(n, per_slot)

        def a_send(s, c):
            if s > 1:
                arrived(ag.at[c, pl.ds(off[s - 1], half >> (s - 1))], ag_r.at[c, s - 1])
            a_part(s, c, 1)

        def a_keep(s, c):
            a_part(s, c, 0)

        def a_close(c):
            arrived(ag.at[c, pl.ds(off[bits - 1], 1)], ag_r.at[c, bits - 1])
            out[0, pl.ds(pl.multiple_of(c * ra, 16), ra), :] = a_sum(bits, c, 0)

        def b_one(p, c, t, slot, j):
            rb, q = rbs[p], p % 2
            acc = product(slot, rb, group_at(c, 0, 1, j))
            src = bsend.at[q, c, t, j, pl.ds(0, rb), :]
            src[...] = acc.astype(BF16)
            remote(src, bg[p].at[c, t, j], b_s.at[q], bg_r[p].at[c, t, 0], across(c, 0)).start()

        def b_first(p, c, t, slot):
            loop(half, lambda j: b_one(p, c, t, slot, j))

        def b_sent(p):
            q = p % 2
            arrived(bsend.at[q, :, :, :, pl.ds(0, rbs[p]), :], b_s.at[q])

        def b_merge(p, c, t, s, add):
            n = half >> (s - 1)
            arrived(bg[p].at[c, t, pl.ds(off[s - 1], n)], bg_r[p].at[c, t, s - 1])

            def per_slot(i):
                h, jj = 1 - i // (n // 2), i % (n // 2)
                j = slot_at(c, s, h, jj)
                bg[p][c, t, off[s - 1] + j] = (add(j) + bg[p][c, t, off[s - 1] + j].astype(F32)).astype(BF16)

                @pl.when(i < n // 2)
                def _():
                    remote(bg[p].at[c, t, off[s - 1] + j], bg[p].at[c, t, off[s] + jj], send.at[3],
                           bg_r[p].at[c, t, s], across(c, s)).start()
            loop(n, per_slot)

        def b_second(p, c, t, slot):
            b_merge(p, c, t, 1, lambda j: product(slot, rbs[p], group_at(c, 0, 0, j)))

        def b_middle(p, t):
            for s in range(2, bits):
                loop(2, lambda c: b_merge(
                    p, c, t, s, lambda j: bg[p][c, t, off[s - 2] + slot_at(c, s - 1, 0, j)].astype(F32)))

        def b_line(p, t):
            rb = rbs[p]
            d = dest(t)

            def body(c):
                tail = off[bits - 1]
                arrived(bg[p].at[c, t, pl.ds(tail, 1)], bg_r[p].at[c, t, bits - 1])
                kept = off[bits - 2] + slot_at(c, bits - 1, 0, 0)

                def val():
                    return bg[p][c, t, tail].astype(F32) + bg[p][c, t, kept].astype(F32)

                feed = choose(feeds, t)
                mid = t < ring - 1

                @pl.when(jnp.logical_and(mid, feed == 0))
                def _():
                    bz[p][c, d] = val().astype(BF16)

                @pl.when(jnp.logical_and(mid, feed == 1))
                def _():
                    arrived(bz[p].at[c, d], bz_r[p].at[c, d])
                    bz[p][c, d] = (val() + bz[p][c, d].astype(F32)).astype(BF16)

                @pl.when(mid)
                def _():
                    land = choose(lands, t)
                    remote(bz[p].at[c, d], bz[p].at[c, land], send.at[4], bz_r[p].at[c, land], toward(t)).start()

                @pl.when(t == ring - 1)
                def _():
                    at = pl.ds(pl.multiple_of(leads[p] + c * rb, 16), rb)
                    out[0, at, :] = val()
                    for there, slot in ((left, z), (right, ring)):
                        @pl.when(there)
                        def _():
                            arrived(bz[p].at[c, slot], bz_r[p].at[c, slot])
                            out[0, at, :] = out[0, at, :] + bz[p][c, slot].astype(F32)
            loop(2, body)

        class Tiles:
            def __init__(self, count, spot, body, first=None, valid=None):
                self.count, self.spot, self.body, self.first = count, spot, body, first
                self.valid = valid or (lambda i: None)

            def guard(self, i, fn):
                ok = self.valid(i)
                if ok is None:
                    fn()
                else:
                    pl.when(ok)(fn)

            def begin(self, i, j, slot):
                def go():
                    tile_own(*self.spot(i, j), slot).start()
                    if self.first is not None:
                        self.first(i, j)
                    tile_other(*self.spot(i, j), slot).start()
                self.guard(i, go)

            def run(self, i, j, slot):
                def go():
                    tile_own(*self.spot(i, j), slot).wait()
                    tile_other(*self.spot(i, j), slot).wait()
                    self.body(i, j, slot)
                self.guard(i, go)

        def b_tiles(p, first, t0=0):
            rb = rbs[p]
            fn = b_first if first else b_second

            def spot(i, j):
                return leads[p] + j * rb, dest(t0 + i), rb, wxb[p].at[j, t0 + i]

            def await_rows(i, j):
                arrived(wxb[p].at[j, t0 + i], wb_r[p].at[j, t0 + i])

            def await_laid(i, j):
                pl.when(i == 0)(lambda: await_rows(i, j))

            await_fn = await_rows if first else await_laid if p == 0 else None
            return Tiles(2, spot, lambda i, j, slot: fn(p, j, t0 + i, slot), await_fn)

        def a_tiles(k0, amount, count):
            def unit(i):
                return k0 + (i * amount) // count - 2 + 2 * ends

            def spot(i, j):
                c, t, _ = a_unit(unit(i))
                return c * ra, dest(t), ra, wxa.at[c, t]

            def await_rows(i, j):
                c, t, hh = a_unit(unit(i))

                @pl.when(hh == 0)
                def _():
                    arrived(wxa.at[c, t], wa_r.at[c, t])

            def valid(i):
                u = unit(i)
                ok = jnp.logical_and(u >= 0, u < n_units)
                return jnp.logical_and(ok, ((i + 1) * amount) // count > (i * amount) // count)

            return Tiles(1, spot, lambda i, j, slot: a_body(unit(i), slot), await_rows, valid)

        def z_step(p, t):
            b_middle(p, t)
            b_line(p, t)

        x_copy.wait_recv()
        code_input(1, xp)
        def laid(c):
            tile_own(leads[0] + c * rbs[0], dest(0), rbs[0], None, c).wait()
            arrived(wt.at[c, 1, :, pl.ds(0, rbs[0]), :], st_r.at[c])

        laid(0)
        b_one(0, 0, 0, 0, 0)
        laid(1)
        b_one(0, 1, 0, 1, 0)
        loop(half - 1, lambda j: b_one(0, 0, 0, 0, j + 1))
        opening = a_tiles(0, 1, 1)
        opening.begin(0, 0, 0)
        loop(half - 1, lambda j: b_one(0, 1, 0, 1, j + 1))

        def push_rest():
            push_both(1)
            loop(ring, lambda t: push_a(1, t))
            for p in range(2, pairs):
                push_both(p)

        sites = [(1, [opening], None), push_rest]
        k0 = 1
        for p in range(pairs):
            final = p == pairs - 1
            for first in (True, False):
                amount = UNITS_A[p][0 if first else 1] * ring // 4
                lead_in = int(p == 0 and first)
                amount -= lead_in
                count = ring - lead_in
                parts = [b_tiles(p, first, lead_in)]
                if amount:
                    parts.append(a_tiles(k0, amount, count))
                    k0 += amount
                post = None
                if first and p >= 2:
                    sites.append(lambda p=p: b_sent(p - 2))
                if not first and p >= 1:
                    def post(i, p=p, final=final):
                        t = i if final else blend(ends, i - 1, i + 1)
                        ok = jnp.logical_and(t >= 0, t < ring - 1)

                        @pl.when(jnp.logical_and(ok, ends == 0) if final else ok)
                        def _():
                            z_step(p - 1, t)
                sites.append((count, parts, post))
                if first and p >= 1:
                    def lead_on(p=p, final=final):
                        @pl.when(ends == 1)
                        def _():
                            loop(ring - 1 if final else 1, lambda t: z_step(p - 1, t))
                    sites.append(lead_on)
                if first and p >= 2:
                    sites.append(lambda p=p: z_step(p - 2, ring - 1))

        def tail():
            last = pairs - 1
            a_spread(0)
            a_spread(1)
            z_step(last, 0)

            def pass_on(mine):
                @pl.when(ends == mine)
                def _():
                    loop(ring - 2, lambda t: z_step(last, t + 1))

            pass_on(1)
            for c in range(2):
                a_send(1, c)
            pass_on(0)
            for c in range(2):
                a_keep(1, c)
            z_step(last - 1, ring - 1)
            for s in range(2, bits):
                for c in range(2):
                    a_send(s, c)
                    a_keep(s, c)
            z_step(last, ring - 1)
            for c in range(2):
                a_close(c)

        sites.append(tail)

        tiled = [site for site in sites if isinstance(site, tuple)]
        seen, parity = 0, 0
        for site in sites:
            if not isinstance(site, tuple):
                site()
                continue
            seen += 1
            follow = tiled[seen][1][0] if seen < len(tiled) else None
            count, parts, post = site
            per = sum(part.count for part in parts)

            def run(i, count=count, parts=parts, post=post, per=per, follow=follow, parity=parity):
                lead = 0
                for q, part in enumerate(parts):
                    def visit(j, q=q, part=part, lead=lead):
                        slot = (parity + i * per + lead + j) % 2

                        @pl.when(j + 1 < part.count)
                        def _():
                            part.begin(i, j + 1, 1 - slot)

                        @pl.when(j + 1 == part.count)
                        def _():
                            if q + 1 < len(parts):
                                parts[q + 1].begin(i, 0, 1 - slot)
                                return

                            @pl.when(i + 1 < count)
                            def _():
                                parts[0].begin(i + 1, 0, 1 - slot)
                            if follow is not None:
                                @pl.when(i + 1 == count)
                                def _():
                                    follow.begin(0, 0, 1 - slot)
                        part.run(i, j, slot)
                    loop(part.count, visit)
                    lead += part.count
                if post is not None:
                    post(i)
            loop(count, run)
            parity = (parity + count * per) % 2

        x_copy.wait_send()
        for p in range(pairs):
            arrived(wxb[p], w_s.at[p])
        arrived(wxa, w_s.at[pairs])
        for c in range(2):
            arrived(stage.at[c], st_s.at[c])
        arrived(az.at[:, pl.ds(0, ring - 1)], send.at[0])
        arrived(ag.at[:, pl.ds(0, half)], send.at[1])
        arrived(ag.at[:, pl.ds(0, half - 1)], send.at[2])
        for p in range(max(0, pairs - 2), pairs):
            b_sent(p)
        for p in range(pairs):
            arrived(bg[p].at[:, :, pl.ds(0, half - 1)], send.at[3])
            arrived(bz[p].at[:, pl.ds(0, ring - 1)], send.at[4])

    dma = pltpu.SemaphoreType.DMA
    shapes = [
        pltpu.VMEM((splits, depth, cols), BF16),
        pltpu.VMEM((splits, depth, cols), BF16),
        pltpu.VMEM((2, blocks, rbs[0], depth), BF16),
        pltpu.VMEM((groups, 2 * depth, cols), BF16),
        pltpu.VMEM((2, 2, blocks, top, depth), BF16),
        pltpu.VMEM((top, 2 * depth), BF16),
        pltpu.VMEM((top, cols), F32),
        pltpu.VMEM((2, ring + 1, groups, ra, cols), BF16),
        pltpu.VMEM((2, groups - 1, ra, cols), BF16),
        pltpu.VMEM((2, 2, ring, half, max(rbs), cols), BF16),
        dma, dma, dma, dma((2,)), dma((2,)), dma((2,)), dma((pairs + 1,)), dma((2, ring)), dma((2, 2)), dma((5,)), dma((2,)),
        dma((2, ring + 1, groups)), dma((2, half)), dma((2, bits)),
    ]
    shapes += [pltpu.VMEM((2, ring, groups - 1, rb, cols), BF16) for rb in rbs]
    shapes += [pltpu.VMEM((2, ring + 1, rb, cols), BF16) for rb in rbs]
    shapes += [dma((2, ring)) for _ in rbs]
    shapes += [dma((2, ring, bits)) for _ in rbs]
    shapes += [dma((2, ring + 1)) for _ in rbs]
    held = [jax.ShapeDtypeStruct((2, ring, blocks, ra, depth), BF16)]
    held += [jax.ShapeDtypeStruct((2, ring, blocks, rb, depth), BF16) for rb in rbs]
    return pl.pallas_call(
        kernel,
        name="coded_share",
        out_shape=(pltpu.VMEM((1, rows, cols), F32), *held),
        in_specs=[
            pl.BlockSpec(memory_space=pltpu.SMEM),
            pl.BlockSpec(memory_space=pl.ANY),
            pl.BlockSpec(memory_space=pl.ANY),
        ],
        out_specs=tuple(pl.BlockSpec(memory_space=m) for m in [pltpu.VMEM] + [pl.ANY] * len(held)),
        scratch_shapes=shapes,
        compiler_params=pltpu.CompilerParams(
            collective_id=0, has_side_effects=True, vmem_limit_bytes=LIMIT),
    )


def split_rows(rows):
    units = rows // 16
    ua = max(1, units * SHARE_A // 128)
    ub = (units - 2 * ua) // 2
    whole = sum(SHARES_B)
    cut = [max(1, ub * share // whole) for share in SHARES_B]
    for i in range(ub - sum(cut)):
        cut[i % len(cut)] += 1
    return 16 * ua, [16 * n for n in cut]


def solution(mesh):
    groups, members = mesh.shape["grp"], mesh.shape["mem"]

    def per_device(weight, activation, points):
        blocks, height, depth = weight.shape
        splits, _, cols = activation.shape
        rows = height // members
        ra, rbs = split_rows(rows)
        call = make_kernel(groups, members, blocks, splits, rows, depth, cols, ra, rbs)
        return call(points, weight, activation)[0]

    placed = (P(None, None, ("grp", "mem")), P(None, ("grp", "mem"), None), P())
    return jax.shard_map(
        per_device, mesh=mesh, in_specs=placed, out_specs=P("grp", "mem", None), check_vma=False)
```
